128 devices in a mesh: rows: 16 (over y, z), trees: 8 (over x, core).
Axes of the slice: x: 4, y: 4, z: 4, core: 2. Of those that a mesh axis runs over, the one named last changes fastest.
Arguments:
- leaf_index: int32 [128, 262144], P(None, ('rows', 'trees')), may hold values from 0 to 31, as said below
- out_of_bag: bfloat16 [128, 262144], P(None, ('rows', 'trees')), may hold values from 0 to 4, as said below
- labels: int32 [262144], P(('rows', 'trees')), may hold values from 0 to 999
Outputs:
- tallies: float32 [128, 32, 1000], P('trees', 'rows')
- tree_error: float32 [128], P('trees')
- forest_error: float32 [], replicated
The draws below stay inside these ranges and needn't reach their ends.
Inputs may be any that keep to these rules, and one draw needn't show every extreme that they name: `out_of_bag`: 0 exactly where a row was in a tree's sample, else at least 0.25. `leaf_index`: in each tree, the 2048 rows of one device reach every leaf exactly 2048 // 32 times.
All inputs are finite; a program needn't handle non-finite values.
Results may differ from the reference program's by a relative error of at most 0.0003.
Values sent between devices are 32-bit elements; how exact they have to be, the bound alone decides.
No kernel may reach another device: no remote copies, remote signals or barrier semaphores. Data moves between devices by JAX's collectives and lax.ppermute only.
A program may use at most 128 MiB of HBM per device.

```python
import math
import jax
import jax.numpy as jnp
from jax import lax

TREES = 128
CLASSES = 1000
LEAVES = 32
ROW_DEV = 2048
ROWS = 262144


def label_leaf_pair(key):
    device_total = ROWS // ROW_DEV
    per_leaf = ROW_DEV // LEAVES
    class_weight = (1 << 20) // (jnp.arange(CLASSES, dtype=jnp.int32) + 1)
    bounds = jnp.cumsum(class_weight).astype(jnp.int32)
    drawn_value = jax.random.randint(jax.random.fold_in(key, 3), (ROWS,), 0, bounds[-1], dtype=jnp.int32)
    rank_class = jnp.searchsorted(bounds, drawn_value, side='right').astype(jnp.int32)
    class_order = jax.random.permutation(jax.random.fold_in(key, 5), CLASSES).astype(jnp.int32)
    labels = jnp.take(class_order, rank_class).astype(jnp.int32)
    tie_keys = jax.random.split(jax.random.fold_in(key, 7), TREES * device_total)
    positions = jnp.arange(ROW_DEV, dtype=jnp.int32)
    shuffled = jax.vmap(lambda single: jax.random.permutation(single, positions))(tie_keys)
    shuffled = shuffled.reshape(TREES, device_total, ROW_DEV).astype(jnp.int32)
    random_leaf = shuffled % LEAVES
    sort_score = labels.reshape(1, device_total, ROW_DEV) * ROW_DEV + shuffled
    sort_order = jnp.argsort(sort_score, axis=2, stable=True).astype(jnp.int32)
    row_rank = jnp.argsort(sort_order, axis=2, stable=True).astype(jnp.int32)
    leaf_keys = jax.random.split(jax.random.fold_in(key, 9), TREES)
    leaf_maps = jax.vmap(lambda single: jax.random.permutation(single, LEAVES))(leaf_keys).astype(jnp.int32)
    sorted_leaf = jax.vmap(lambda mapping, ranks: jnp.take(mapping, ranks // per_leaf))(leaf_maps, row_rank)
    picked = jax.random.permutation(jax.random.fold_in(key, 13), TREES) < TREES // 2
    leaf_final = jnp.where(picked[:, None, None], sorted_leaf, random_leaf)
    return (labels, leaf_final.reshape(TREES, ROWS).astype(jnp.int32))


def draw_labels(key, part):
    return label_leaf_pair(key)[0]


def draw_leaf_index(key, part):
    return label_leaf_pair(key)[1]


def draw_out_of_bag(key, part):
    marks_drawn = jax.random.randint(jax.random.fold_in(key, 11), (TREES, ROWS), 0, 1000, dtype=jnp.int32)
    position = jnp.arange(ROWS, dtype=jnp.int32)
    level = 200 + 400 * position // ROWS
    sizes = jnp.exp(jax.random.uniform(jax.random.fold_in(key, 17), (TREES, ROWS), jnp.float32, math.log(0.25), math.log(4.0)))
    return jnp.where(marks_drawn < level[None, :], sizes, 0.0).astype(jnp.bfloat16)


def setup_inputs(seed: int = 0) -> dict:
    arg_keys = jax.random.split(jax.random.key(seed), 4)
    leaf_index = draw_leaf_index(jax.random.fold_in(arg_keys[3], 71), 0)
    out_of_bag = draw_out_of_bag(jax.random.fold_in(arg_keys[3], 71), 0)
    labels = draw_labels(jax.random.fold_in(arg_keys[3], 71), 0)
    return {"leaf_index": leaf_index, "out_of_bag": out_of_bag, "labels": labels}


def reference(leaf_index, out_of_bag, labels):
    def one_tree(tree_pair):
        leaves_row, weight_row = tree_pair
        slot_index = leaves_row * CLASSES + labels
        counts = jax.ops.segment_sum(weight_row.astype(jnp.float32), slot_index, num_segments=LEAVES * CLASSES)
        return counts.reshape(LEAVES, CLASSES)

    tallies = lax.map(one_tree, (leaf_index, out_of_bag))
    leaf_total = jnp.sum(tallies, axis=2)
    leaf_top = jnp.max(tallies, axis=2)
    wrong_sum = jnp.sum(leaf_total - leaf_top, axis=1)
    seen_sum = jnp.sum(leaf_total, axis=1)
    tree_error = wrong_sum / seen_sum
    forest_error = jnp.sum(wrong_sum) / jnp.sum(seen_sum)
    return tallies, tree_error, forest_error
```

```python
import functools

import jax
import jax.numpy as jnp
from jax import lax
from jax.experimental import pallas as pl
from jax.experimental.pallas import tpu as pltpu
from jax.sharding import Mesh
from jax.sharding import PartitionSpec as P

CLASSES = 1000
LEAVES = 32
TREES_ALL = 128
ROW_DEV = 2048
N_DEV = 128
N_ROWS = 16
N_TREES = 8
RANKS = ROW_DEV // LEAVES
ROWS = ("rows_0", "rows_1")
TREES = ("trees_0", "trees_1")
ALL = ROWS + TREES

OCT = 8
PAIRS = OCT // 2
CHUNKS = 2
CHUNK_ROWS = PAIRS * 4
BLOCK = 256
N_BLOCK = ROW_DEV // BLOCK
WORDS = 11
VMEM = 56 * 1024 * 1024

F32 = jnp.float32
BF16 = jnp.bfloat16


def iota16(shape):
    return lax.broadcasted_iota(jnp.int32, shape, 0).astype(F32).astype(BF16)


def pack_kernel(half, leaf_ref, oob_ref, lab_ref, out_ref, leaf_s, w_s, rank_s, enc_s):
    lab = lab_ref[...]
    enc = lax.shift_left(128 + (lab & 127), lab >> 7).astype(F32)
    enc_s[...] = jnp.broadcast_to(enc, (16, ROW_DEV)).astype(BF16)
    tri = (
        lax.broadcasted_iota(jnp.int32, (BLOCK, BLOCK), 0)
        <= lax.broadcasted_iota(jnp.int32, (BLOCK, BLOCK), 1)
    ).astype(F32).astype(BF16)
    row16 = iota16((16, ROW_DEV))
    zero = jnp.zeros((16, ROW_DEV), BF16)
    one = jnp.ones((16, ROW_DEV), BF16)
    low = lax.broadcasted_iota(jnp.int32, (LEAVES, 128), 1) < RANKS

    def octet(g, carry):
        leaf = leaf_ref[g, pl.ds(half * OCT, OCT), :]
        w = oob_ref[g, pl.ds(half * OCT, OCT), :].astype(F32)
        word = (leaf * 171) >> 9
        field = leaf - 3 * word
        unit = jnp.where(field == 0, 1.0, jnp.where(field == 1, 128.0, 16384.0))
        held = [jnp.where(word == j, unit, 0.0) for j in range(WORDS)]
        marks = jnp.concatenate(
            [held[j][:, b * BLOCK : (b + 1) * BLOCK] for j in range(WORDS) for b in range(N_BLOCK)],
            axis=0,
        ).astype(BF16)
        counts = jnp.dot(marks, tri, preferred_element_type=F32)
        picked = [jnp.zeros((OCT, BLOCK), F32) for _ in range(N_BLOCK)]
        for j in range(WORDS):
            before = jnp.zeros((OCT, BLOCK), F32)
            for b in range(N_BLOCK):
                at = (j * N_BLOCK + b) * OCT
                here = counts[at : at + OCT]
                mine = word[:, b * BLOCK : (b + 1) * BLOCK] == j
                picked[b] = jnp.where(mine, here + before, picked[b])
                if b + 1 < N_BLOCK:
                    before = before + jnp.broadcast_to(here[:, BLOCK - 1 :], (OCT, BLOCK))
        number = jnp.concatenate(picked, axis=1).astype(jnp.int32)
        rank = ((number >> (7 * field)) & 127) - 1
        leaf_s[...] = leaf.astype(F32)
        w_s[...] = w
        rank_s[...] = rank.astype(F32)
        enc_b = enc_s[...]
        for pair in range(PAIRS):
            placed = []
            for t in (2 * pair, 2 * pair + 1):
                leaf_b = jnp.broadcast_to(leaf_s[t : t + 1, :], (16, ROW_DEV)).astype(BF16)
                w_b = jnp.broadcast_to(w_s[t : t + 1, :], (16, ROW_DEV)).astype(BF16)
                rank_b = jnp.broadcast_to(rank_s[t : t + 1, :], (16, ROW_DEV)).astype(BF16)
                at_leaf = [leaf_b == (row16 + 16 * i) for i in range(2)]
                lhs = jnp.concatenate(
                    [jnp.where(m, w_b, zero) for m in at_leaf] + [jnp.where(m, enc_b, zero) for m in at_leaf],
                    axis=0,
                )
                rhs = jnp.concatenate(
                    [jnp.where(rank_b == (row16 + 16 * i), one, zero) for i in range(4)], axis=0
                )
                placed.append(
                    lax.dot_general(lhs, rhs, (((1,), (1,)), ((), ())), preferred_element_type=F32)
                )
            both = jnp.concatenate(placed, axis=1)
            weights = both[:LEAVES]
            code = both[LEAVES:].astype(jnp.int32)
            high = 24 - lax.clz(code)
            label = ((code >> high) + (high - 1) * 128).astype(F32)
            for p in range(N_ROWS):
                out_ref[p, g, 4 * pair : 4 * pair + 2, :] = weights[2 * p : 2 * p + 2]
                out_ref[p, g, 4 * pair + 2 : 4 * pair + 4, :] = label[2 * p : 2 * p + 2]
        return carry

    lax.fori_loop(0, N_TREES, octet, 0)


def pack(half, leaf_index, out_of_bag, labels):
    return pl.pallas_call(
        functools.partial(pack_kernel, half),
        out_shape=jax.ShapeDtypeStruct((N_ROWS, N_TREES, CHUNK_ROWS, 128), F32),
        scratch_shapes=[
            pltpu.VMEM((OCT, ROW_DEV), F32),
            pltpu.VMEM((OCT, ROW_DEV), F32),
            pltpu.VMEM((OCT, ROW_DEV), F32),
            pltpu.VMEM((16, ROW_DEV), BF16),
        ],
        compiler_params=pltpu.CompilerParams(vmem_limit_bytes=VMEM),
        cost_estimate=pl.CostEstimate(flops=4_000_000_000, bytes_accessed=3_000_000, transcendentals=0),
        name=f"pack_{half}",
    )(
        leaf_index.reshape(N_TREES, 16, ROW_DEV),
        out_of_bag.reshape(N_TREES, 16, ROW_DEV),
        labels.reshape(1, ROW_DEV),
    )


GROUPS = OCT * 2
HALF_DEV = N_DEV // 2


def tally_kernel(in_ref, out_ref, wrong_ref, seen_ref, w_s, hi_s, lo_s):
    low = lax.broadcasted_iota(jnp.int32, (HALF_DEV, 128), 1) < RANKS
    row16 = iota16((16, 128))
    zero = jnp.zeros((16, 128), BF16)
    one = jnp.ones((16, 128), BF16)

    def halves(row):
        a = in_ref[0:HALF_DEV, row, :]
        b = in_ref[HALF_DEV:N_DEV, row, :]
        return (
            jnp.where(low, a, pltpu.roll(b, RANKS, 1)),
            jnp.where(low, pltpu.roll(a, RANKS, 1), b),
        )

    for pair in range(PAIRS):
        for leaf in range(2):
            w2 = halves(4 * pair + leaf)
            lab2 = halves(4 * pair + 2 + leaf)
            for odd in range(2):
                hi = jnp.floor(lab2[odd] * (1.0 / 32.0))
                w_s[...] = w2[odd]
                hi_s[...] = hi
                lo_s[...] = lab2[odd] - 32.0 * hi
                lhs, rhs = [], []
                for r in range(HALF_DEV):
                    w_b = jnp.broadcast_to(w_s[r : r + 1, :], (16, 128)).astype(BF16)
                    hi_b = jnp.broadcast_to(hi_s[r : r + 1, :], (16, 128)).astype(BF16)
                    lo_b = jnp.broadcast_to(lo_s[r : r + 1, :], (16, 128)).astype(BF16)
                    lhs.append(
                        jnp.concatenate([jnp.where(hi_b == row16 + 16 * i, w_b, zero) for i in range(2)], axis=0)
                    )
                    rhs.append(
                        jnp.concatenate([jnp.where(lo_b == row16 + 16 * i, one, zero) for i in range(2)], axis=0)
                    )
                table = lax.dot_general(
                    jnp.concatenate(lhs, axis=1),
                    jnp.concatenate(rhs, axis=1),
                    (((1,), (1,)), ((), ())),
                    preferred_element_type=F32,
                )
                group = (2 * pair + odd) * 2 + leaf
                out_ref[group] = table
                total = jnp.sum(jnp.sum(table, axis=0, keepdims=True), axis=1, keepdims=True)
                top = jnp.max(jnp.max(table, axis=0, keepdims=True), axis=1, keepdims=True)
                seen_ref[group : group + 1, :] = jnp.broadcast_to(total, (1, 128))
                wrong_ref[group : group + 1, :] = jnp.broadcast_to(total - top, (1, 128))


def tally(received):
    return pl.pallas_call(
        tally_kernel,
        out_shape=(
            jax.ShapeDtypeStruct((GROUPS, 32, 32), F32),
            jax.ShapeDtypeStruct((GROUPS, 128), F32),
            jax.ShapeDtypeStruct((GROUPS, 128), F32),
        ),
        scratch_shapes=[pltpu.VMEM((HALF_DEV, 128), F32)] * 3,
        compiler_params=pltpu.CompilerParams(vmem_limit_bytes=VMEM),
        cost_estimate=pl.CostEstimate(flops=2_000_000_000, bytes_accessed=2_000_000, transcendentals=0),
        name="tally",
    )(received)


def per_device(leaf_index, out_of_bag, labels):
    tables, wrongs, seens = [], [], []
    sent = []
    for half in range(CHUNKS):
        packed = pack(half, leaf_index, out_of_bag, labels)
        packed = packed.reshape(N_DEV, CHUNK_ROWS, 128)
        sent.append(lax.all_to_all(packed, ALL, 0, 0, tiled=True))
    for part in sent:
        table, wrong, seen = tally(part)
        tables.append(table.reshape(OCT, 2, 1024)[:, :, :CLASSES])
        wrongs.append(wrong[:, 0].reshape(OCT, 2).sum(1))
        seens.append(seen[:, 0].reshape(OCT, 2).sum(1))
    wrong = jnp.concatenate(wrongs)
    seen = jnp.concatenate(seens)
    mine = (jnp.arange(N_DEV, dtype=jnp.int32) % N_TREES == lax.axis_index(TREES))[:, None]
    per_tree = jnp.concatenate([wrong, seen])
    pooled = jnp.stack([jnp.sum(wrong), jnp.sum(seen)])
    message = jnp.concatenate(
        [
            jnp.where(mine, per_tree[None, :], 0.0),
            jnp.broadcast_to(pooled[None, :], (N_DEV, 2)),
            jnp.zeros((N_DEV, 94), F32),
        ],
        axis=1,
    )
    sums = jnp.sum(lax.all_to_all(message, ALL, 0, 0, tiled=True), axis=0)
    tree_error = sums[0:16] / sums[16:32]
    forest_error = sums[32] / sums[33]
    return jnp.concatenate(tables, axis=0), tree_error, forest_error


def solution(mesh):
    split = Mesh(mesh.devices.reshape(4, 4, 4, 2), ALL)
    return jax.shard_map(
        per_device,
        mesh=split,
        in_specs=(P(None, ALL), P(None, ALL), P(ALL)),
        out_specs=(P(TREES, ROWS, None), P(TREES), P()),
        check_vma=False,
    )
```

```python
import jax
import jax.numpy as jnp
from jax import lax
from jax.experimental import pallas as pl
from jax.experimental.pallas import tpu as pltpu
from jax.sharding import Mesh
from jax.sharding import PartitionSpec as P

CLASSES = 1000
LEAVES = 32
TREES_ALL = 128
ROW_DEV = 2048
N_DEV = 128
N_ROWS = 16
N_TREES = 8
GROUP = TREES_ALL // N_TREES
RANKS = ROW_DEV // LEAVES
ROWS = ("rows_0", "rows_1")
TREES = ("trees_0", "trees_1")
ALL = ROWS + TREES
REGS = ROW_DEV // 8
HALF_DEV = N_DEV // 2

F32 = jnp.float32
BF16 = jnp.bfloat16
I32 = jnp.int32


def ordered(x, i, j):
    x[i], x[j] = jnp.minimum(x[i], x[j]), jnp.maximum(x[i], x[j])


COPIES = 4
SPAN = ROW_DEV // COPIES
LEAF_STEP = float(1 << 20)


def pack_kernel(leaf_hbm, oob_hbm, lab_ref, out_hbm, s_ref, leaf_ref, oob_ref, out_ref, leaf_sem, oob_sem, out_sem):
    sub = lax.broadcasted_iota(I32, (8, 128), 0)

    def loads(c):
        cols = pl.ds(c * SPAN, SPAN)
        return (
            pltpu.make_async_copy(leaf_hbm.at[:, cols], leaf_ref.at[c], leaf_sem.at[c]),
            pltpu.make_async_copy(oob_hbm.at[:, cols], oob_ref.at[c], oob_sem.at[c]),
        )

    for c in range(COPIES):
        for copy in loads(c):
            copy.start()

    def get(v):
        return s_ref[pl.ds(pl.multiple_of(v * 8, 8), 8), :]

    def put(v, x):
        s_ref[pl.ds(pl.multiple_of(v * 8, 8), 8), :] = x

    def sort_32(b, carry):
        x = [get(b * 32 + r) for r in range(32)]
        for k in range(1, 6):
            for i in range(32):
                j = i ^ ((1 << k) - 1)
                if i < j:
                    ordered(x, i, j)
            for d in reversed(range(k - 1)):
                for i in range(32):
                    if not i & (1 << d):
                        ordered(x, i, i | (1 << d))
        for r in range(32):
            put(b * 32 + r, x[r])
        return carry

    for c in range(COPIES):
        for copy in loads(c):
            copy.wait()
        for q in range(SPAN // 128):
            cols = pl.ds(q * 128, 128)
            w = oob_ref[c, :, cols].astype(F32) * 512.0
            code = jnp.minimum(
                jnp.minimum(w, w * 0.5 + 128.0), jnp.minimum(w * 0.25 + 256.0, w * 0.125 + 384.0)
            )
            high = (leaf_ref[c, :, cols] - 16).astype(F32) * LEAF_STEP
            label = lab_ref[:, pl.ds(c * SPAN + q * 128, 128)].astype(F32)
            key = high + (code * 1024.0 + label)
            s_ref[pl.ds(c * SPAN + q * 128, 128), :] = jnp.transpose(key)
        lax.fori_loop(c * SPAN // 256, (c + 1) * SPAN // 256, sort_32, 0)

    def low_bits(b, carry):
        x = [get(b * 32 + r) for r in range(32)]
        for d in reversed(range(5)):
            for i in range(32):
                if not i & (1 << d):
                    ordered(x, i, i | (1 << d))
        for r in range(32):
            put(b * 32 + r, x[r])
        return carry

    def swapped(x, flip):
        return jnp.take_along_axis(x, sub ^ flip, axis=0, mode="promise_in_bounds")

    def across(x, y, bit):
        return jnp.where(sub & bit == 0, jnp.minimum(x, y), jnp.maximum(x, y))

    def high_bits(k):
        top = min(k, 8)
        bits = list(range(5, top))
        n = 1 << len(bits)
        per_block = 16
        blocks = REGS >> top

        def body(t, carry):
            block, low = t // per_block, t % per_block
            base = block << top
            at = [base + (h << 5) + low for h in range(n)] + [base + (h << 5) + (31 - low) for h in range(n)]
            x = [get(v) for v in at]
            mirror = lambda e: (n - 1 - e % n) + (n if e < n else 0)
            if k <= 8:
                for e in range(n):
                    if e & (n >> 1):
                        continue
                    ordered(x, e, mirror(e))
                    ordered(x, e + n, mirror(e + n))
            else:
                flip = (1 << (k - 8)) - 1
                x = [across(x[e], swapped(x[mirror(e)], flip), 1 << (k - 9)) for e in range(2 * n)]
                for d in reversed(range(k - 9)):
                    x = [across(v, swapped(v, 1 << d), 1 << d) for v in x]
            first = len(bits) - 2 if k <= 8 else len(bits) - 1
            for d in reversed(range(first + 1)):
                for e in range(2 * n):
                    if not e & (1 << d):
                        ordered(x, e, e | (1 << d))
            for v, val in zip(at, x):
                put(v, val)
            return carry

        lax.fori_loop(0, blocks * per_block, body, 0, unroll=UNROLL[k])

    for k in range(6, 12):
        high_bits(k)
        lax.fori_loop(0, REGS // 32, low_bits, 0)

    def stored(p):
        return pltpu.make_async_copy(out_ref.at[p], out_hbm.at[p], out_sem.at[p])

    odd = (lax.broadcasted_iota(I32, (1, 128), 1) >= RANKS).astype(F32)
    for p in range(N_ROWS):
        start = (p % 2) * 1024 + p // 2
        key = jnp.transpose(s_ref[pl.ds(start, 128, stride=8), :])
        rest = key - (odd + float(2 * p - 16)) * LEAF_STEP
        code = jnp.floor(rest * (1.0 / 1024.0))
        label = rest - code * 1024.0
        w = jnp.maximum(
            jnp.maximum(code, code * 2.0 - 256.0), jnp.maximum(code * 4.0 - 1024.0, code * 8.0 - 3072.0)
        ) * (1.0 / 512.0)
        out_ref[p, :, 0] = w.reshape(N_TREES, GROUP, 128)
        out_ref[p, :, 1] = label.reshape(N_TREES, GROUP, 128)
        stored(p).start()
    for p in range(N_ROWS):
        stored(p).wait()


UNROLL = {6: 4, 7: 2, 8: 1, 9: 1, 10: 1, 11: 1}


def pack(leaf_index, out_of_bag, labels):
    return pl.pallas_call(
        pack_kernel,
        in_specs=[
            pl.BlockSpec(memory_space=pltpu.HBM),
            pl.BlockSpec(memory_space=pltpu.HBM),
            pl.BlockSpec(memory_space=pltpu.VMEM),
        ],
        out_specs=pl.BlockSpec(memory_space=pltpu.HBM),
        out_shape=jax.ShapeDtypeStruct((N_ROWS, N_TREES, 2, GROUP, 128), F32),
        scratch_shapes=[
            pltpu.VMEM((ROW_DEV, 128), F32),
            pltpu.VMEM((COPIES, TREES_ALL, SPAN), I32),
            pltpu.VMEM((COPIES, TREES_ALL, SPAN), BF16),
            pltpu.VMEM((N_ROWS, N_TREES, 2, GROUP, 128), F32),
            pltpu.SemaphoreType.DMA((COPIES,)),
            pltpu.SemaphoreType.DMA((COPIES,)),
            pltpu.SemaphoreType.DMA((N_ROWS,)),
        ],
        compiler_params=pltpu.CompilerParams(vmem_limit_bytes=60 * 1024 * 1024),
        cost_estimate=pl.CostEstimate(flops=40_000_000, bytes_accessed=3_700_000, transcendentals=0),
        name="pack",
    )(leaf_index, out_of_bag, labels.reshape(1, ROW_DEV))


def iota16(shape):
    return lax.broadcasted_iota(I32, shape, 0).astype(F32).astype(BF16)


def tally_kernel(in_ref, table_ref, message_ref, w_s, hi_s, lo_s, sum_s, top_s):
    low16 = lax.broadcasted_iota(I32, (GROUP, 128), 1) < RANKS
    row16 = iota16((16, 128))
    zero = jnp.zeros((16, 128), BF16)
    one = jnp.ones((16, 128), BF16)

    def halves(a, b):
        return (
            jnp.where(low16, a, pltpu.roll(b, RANKS, 1)),
            jnp.where(low16, pltpu.roll(a, RANKS, 1), b),
        )

    def spread(s, carry):
        w2 = halves(in_ref[s, 0], in_ref[s + HALF_DEV, 0])
        lab2 = halves(in_ref[s, 1], in_ref[s + HALF_DEV, 1])
        for leaf in range(2):
            hi = jnp.floor(lab2[leaf] * (1.0 / 32.0))
            w_s[leaf, s] = w2[leaf]
            hi_s[leaf, s] = hi
            lo_s[leaf, s] = lab2[leaf] - 32.0 * hi
        return carry

    lax.fori_loop(0, HALF_DEV, spread, 0, unroll=4)

    def tree(t, carry):
        for leaf in range(2):
            lhs, rhs = [], []
            for r in range(HALF_DEV):
                w_b = jnp.broadcast_to(w_s[leaf, r, pl.ds(t, 1), :], (16, 128)).astype(BF16)
                hi_b = jnp.broadcast_to(hi_s[leaf, r, pl.ds(t, 1), :], (16, 128)).astype(BF16)
                lo_b = jnp.broadcast_to(lo_s[leaf, r, pl.ds(t, 1), :], (16, 128)).astype(BF16)
                lhs.append(jnp.concatenate([jnp.where(hi_b == row16 + 16 * i, w_b, zero) for i in range(2)], axis=0))
                rhs.append(jnp.concatenate([jnp.where(lo_b == row16 + 16 * i, one, zero) for i in range(2)], axis=0))
            table = lax.dot_general(
                jnp.concatenate(lhs, axis=1),
                jnp.concatenate(rhs, axis=1),
                (((1,), (1,)), ((), ())),
                preferred_element_type=F32,
            )
            table_ref[leaf, t] = table
            sum_s[leaf, pl.ds(t, 1), :] = jnp.sum(table, axis=0, keepdims=True)
            top_s[leaf, pl.ds(t, 1), :] = jnp.max(table, axis=0, keepdims=True)
        return carry

    lax.fori_loop(0, GROUP, tree, 0, unroll=4)
    seen = jnp.zeros((GROUP, 1), F32)
    wrong = jnp.zeros((GROUP, 1), F32)
    for leaf in range(2):
        total = jnp.sum(sum_s[leaf], axis=1, keepdims=True)
        seen = seen + total
        wrong = wrong + (total - jnp.max(top_s[leaf], axis=1, keepdims=True))
    lane = lax.broadcasted_iota(I32, (GROUP, 128), 1)
    row = lax.broadcasted_iota(I32, (GROUP, 128), 0)
    placed = jnp.where(lane == row, wrong, 0.0) + jnp.where(lane == row + GROUP, seen, 0.0)
    message_ref[...] = jnp.broadcast_to(jnp.sum(placed, axis=0, keepdims=True), (N_DEV, 128))


def tally(received):
    return pl.pallas_call(
        tally_kernel,
        out_shape=(
            jax.ShapeDtypeStruct((2, GROUP, 32, 32), F32),
            jax.ShapeDtypeStruct((N_DEV, 128), F32),
        ),
        scratch_shapes=[pltpu.VMEM((2, HALF_DEV, GROUP, 128), F32)] * 3 + [pltpu.VMEM((2, GROUP, 32), F32)] * 2,
        compiler_params=pltpu.CompilerParams(vmem_limit_bytes=16 * 1024 * 1024),
        cost_estimate=pl.CostEstimate(flops=4_000_000_000, bytes_accessed=2_500_000, transcendentals=0),
        name="tally",
    )(received)


def errors_kernel(group_ref, in_ref, tree_ref, forest_ref):
    got = in_ref[...]
    source = lax.broadcasted_iota(I32, (N_DEV, 128), 0)
    mine = jnp.sum(jnp.where(source % N_TREES == group_ref[0], got, 0.0), axis=0, keepdims=True)
    every = jnp.sum(got, axis=0, keepdims=True)
    lane = lax.broadcasted_iota(I32, (1, 128), 1)
    wrong = jnp.sum(jnp.where(lane < GROUP, every, 0.0), axis=1, keepdims=True)
    seen = jnp.sum(jnp.where((lane >= GROUP) & (lane < 2 * GROUP), every, 0.0), axis=1, keepdims=True)
    ratio = mine / pltpu.roll(mine, 128 - GROUP, 1)
    tree_ref[...] = ratio[:, :GROUP]
    forest_ref[...] = wrong / seen


def errors(group, received):
    return pl.pallas_call(
        errors_kernel,
        in_specs=[pl.BlockSpec(memory_space=pltpu.SMEM), pl.BlockSpec(memory_space=pltpu.VMEM)],
        out_shape=(
            jax.ShapeDtypeStruct((1, GROUP), F32),
            jax.ShapeDtypeStruct((1, 1), F32),
        ),
        compiler_params=pltpu.CompilerParams(vmem_limit_bytes=4 * 1024 * 1024),
        name="errors",
    )(group, received)


def per_device(leaf_index, out_of_bag, labels):
    packed = pack(leaf_index, out_of_bag, labels).reshape(N_DEV, 2, GROUP, 128)
    received = lax.all_to_all(packed, ALL, 0, 0, tiled=True)
    table, message = tally(received)
    sums = lax.all_to_all(message, ALL, 0, 0, tiled=True)
    group = lax.axis_index(TREES).astype(I32).reshape(1)
    tree_error, forest_error = errors(group, sums)
    tallies = jnp.swapaxes(table.reshape(2, GROUP, 1024), 0, 1)[:, :, :CLASSES]
    return tallies, tree_error.reshape(GROUP), forest_error.reshape(())


def solution(mesh):
    split = Mesh(mesh.devices.reshape(4, 4, 4, 2), ALL)
    return jax.shard_map(
        per_device,
        mesh=split,
        in_specs=(P(None, ALL), P(None, ALL), P(ALL)),
        out_specs=(P(TREES, ROWS, None), P(TREES), P()),
        check_vma=False,
    )
```

```python
import jax
import jax.numpy as jnp
from jax import lax
from jax.experimental import pallas as pl
from jax.experimental.pallas import tpu as pltpu
from jax.sharding import Mesh
from jax.sharding import PartitionSpec as P

CLASSES = 1000
LEAVES = 32
TREES_ALL = 128
ROW_DEV = 2048
N_DEV = 128
N_ROWS = 16
N_TREES = 8
GROUP = TREES_ALL // N_TREES
RANKS = ROW_DEV // LEAVES
ROWS = ("rows_0", "rows_1")
TREES = ("trees_0", "trees_1")
ALL = ROWS + TREES
REGS = ROW_DEV // 8
HALF_DEV = N_DEV // 2

F32 = jnp.float32
BF16 = jnp.bfloat16
I32 = jnp.int32


def ordered(x, i, j):
    x[i], x[j] = jnp.minimum(x[i], x[j]), jnp.maximum(x[i], x[j])


COPIES = 4
SPAN = ROW_DEV // COPIES
LEAF_STEP = float(1 << 20)


def pack_kernel(leaf_hbm, oob_hbm, lab_ref, out_hbm, s_ref, leaf_ref, oob_ref, out_ref, leaf_sem, oob_sem, out_sem):
    sub = lax.broadcasted_iota(I32, (8, 128), 0)

    def loads(c):
        cols = pl.ds(c * SPAN, SPAN)
        return (
            pltpu.make_async_copy(leaf_hbm.at[:, cols], leaf_ref.at[c], leaf_sem.at[c]),
            pltpu.make_async_copy(oob_hbm.at[:, cols], oob_ref.at[c], oob_sem.at[c]),
        )

    for c in range(COPIES):
        for copy in loads(c):
            copy.start()

    def get(v):
        return s_ref[pl.ds(pl.multiple_of(v * 8, 8), 8), :]

    def put(v, x):
        s_ref[pl.ds(pl.multiple_of(v * 8, 8), 8), :] = x

    def sort_32(b, carry):
        x = [get(b * 32 + r) for r in range(32)]
        for k in range(1, 6):
            for i in range(32):
                j = i ^ ((1 << k) - 1)
                if i < j:
                    ordered(x, i, j)
            for d in reversed(range(k - 1)):
                for i in range(32):
                    if not i & (1 << d):
                        ordered(x, i, i | (1 << d))
        for r in range(32):
            put(b * 32 + r, x[r])
        return carry

    for c in range(COPIES):
        for copy in loads(c):
            copy.wait()
        for q in range(SPAN // 128):
            cols = pl.ds(q * 128, 128)
            w = oob_ref[c, :, cols].astype(F32) * 512.0
            code = jnp.minimum(
                jnp.minimum(w, w * 0.5 + 128.0), jnp.minimum(w * 0.25 + 256.0, w * 0.125 + 384.0)
            )
            high = (leaf_ref[c, :, cols] - 16).astype(F32) * LEAF_STEP
            label = lab_ref[:, pl.ds(c * SPAN + q * 128, 128)].astype(F32)
            key = high + (code * 1024.0 + label)
            s_ref[pl.ds(c * SPAN + q * 128, 128), :] = jnp.transpose(key)
        lax.fori_loop(c * SPAN // 256, (c + 1) * SPAN // 256, sort_32, 0, unroll=True)

    def low_bits(b, carry):
        x = [get(b * 32 + r) for r in range(32)]
        for d in reversed(range(5)):
            for i in range(32):
                if not i & (1 << d):
                    ordered(x, i, i | (1 << d))
        for r in range(32):
            put(b * 32 + r, x[r])
        return carry

    def swapped(x, flip):
        return jnp.take_along_axis(x, sub ^ flip, axis=0, mode="promise_in_bounds")

    def across(x, y, bit):
        return jnp.where(sub & bit == 0, jnp.minimum(x, y), jnp.maximum(x, y))

    def high_bits(k):
        top = min(k, 8)
        bits = list(range(5, top))
        n = 1 << len(bits)
        per_block = 16
        blocks = REGS >> top

        def body(t, carry):
            block, low = t // per_block, t % per_block
            base = block << top
            at = [base + (h << 5) + low for h in range(n)] + [base + (h << 5) + (31 - low) for h in range(n)]
            x = [get(v) for v in at]
            mirror = lambda e: (n - 1 - e % n) + (n if e < n else 0)
            if k <= 8:
                for e in range(n):
                    if e & (n >> 1):
                        continue
                    ordered(x, e, mirror(e))
                    ordered(x, e + n, mirror(e + n))
            else:
                flip = (1 << (k - 8)) - 1
                x = [across(x[e], swapped(x[mirror(e)], flip), 1 << (k - 9)) for e in range(2 * n)]
                for d in reversed(range(k - 9)):
                    x = [across(v, swapped(v, 1 << d), 1 << d) for v in x]
            first = len(bits) - 2 if k <= 8 else len(bits) - 1
            for d in reversed(range(1 if k == 11 else 0, first + 1)):
                for e in range(2 * n):
                    if not e & (1 << d):
                        ordered(x, e, e | (1 << d))
            for v, val in zip(at, x):
                put(v, val)
            return carry

        lax.fori_loop(0, blocks * per_block, body, 0, unroll=True)

    for k in range(6, 11):
        high_bits(k)
        lax.fori_loop(0, REGS // 32, low_bits, 0, unroll=True)
    high_bits(11)

    def stored(p):
        return pltpu.make_async_copy(out_ref.at[p], out_hbm.at[p], out_sem.at[p])

    odd = (lax.broadcasted_iota(I32, (1, 128), 1) >= RANKS).astype(F32)
    for p in range(N_ROWS):
        start = (p % 2) * 1024 + p // 2
        key = jnp.transpose(s_ref[pl.ds(start, 128, stride=8), :])
        rest = key - (odd + float(2 * p - 16)) * LEAF_STEP
        code = jnp.floor(rest * (1.0 / 1024.0))
        label = rest - code * 1024.0
        w = jnp.maximum(
            jnp.maximum(code, code * 2.0 - 256.0), jnp.maximum(code * 4.0 - 1024.0, code * 8.0 - 3072.0)
        ) * (1.0 / 512.0)
        out_ref[p, :, 0] = w.reshape(N_TREES, GROUP, 128)
        out_ref[p, :, 1] = label.reshape(N_TREES, GROUP, 128)
        stored(p).start()
    for p in range(N_ROWS):
        stored(p).wait()


def pack(leaf_index, out_of_bag, labels):
    return pl.pallas_call(
        pack_kernel,
        in_specs=[
            pl.BlockSpec(memory_space=pltpu.HBM),
            pl.BlockSpec(memory_space=pltpu.HBM),
            pl.BlockSpec(memory_space=pltpu.VMEM),
        ],
        out_specs=pl.BlockSpec(memory_space=pltpu.HBM),
        out_shape=jax.ShapeDtypeStruct((N_ROWS, N_TREES, 2, GROUP, 128), F32),
        scratch_shapes=[
            pltpu.VMEM((ROW_DEV, 128), F32),
            pltpu.VMEM((COPIES, TREES_ALL, SPAN), I32),
            pltpu.VMEM((COPIES, TREES_ALL, SPAN), BF16),
            pltpu.VMEM((N_ROWS, N_TREES, 2, GROUP, 128), F32),
            pltpu.SemaphoreType.DMA((COPIES,)),
            pltpu.SemaphoreType.DMA((COPIES,)),
            pltpu.SemaphoreType.DMA((N_ROWS,)),
        ],
        compiler_params=pltpu.CompilerParams(vmem_limit_bytes=60 * 1024 * 1024),
        cost_estimate=pl.CostEstimate(flops=40_000_000, bytes_accessed=3_700_000, transcendentals=0),
        name="pack",
    )(leaf_index, out_of_bag, labels.reshape(1, ROW_DEV))


def iota16(shape):
    return lax.broadcasted_iota(I32, shape, 0).astype(F32).astype(BF16)


def tally_kernel(in_ref, table_ref, message_ref, w_s, hi_s, lo_s, sum_s, top_s):
    low16 = lax.broadcasted_iota(I32, (GROUP, 128), 1) < RANKS
    row16 = iota16((16, 128))
    zero = jnp.zeros((16, 128), BF16)
    one = jnp.ones((16, 128), BF16)

    def halves(a, b):
        return (
            jnp.where(low16, a, pltpu.roll(b, RANKS, 1)),
            jnp.where(low16, pltpu.roll(a, RANKS, 1), b),
        )

    def spread(s, carry):
        w2 = halves(in_ref[s, 0], in_ref[s + HALF_DEV, 0])
        lab2 = halves(in_ref[s, 1], in_ref[s + HALF_DEV, 1])
        for leaf in range(2):
            hi = jnp.floor(lab2[leaf] * (1.0 / 32.0))
            w_s[leaf, s] = w2[leaf]
            hi_s[leaf, s] = hi
            lo_s[leaf, s] = lab2[leaf] - 32.0 * hi
        return carry

    lax.fori_loop(0, HALF_DEV, spread, 0, unroll=True)

    def tree(t, carry):
        for leaf in range(2):
            lhs, rhs = [], []
            for r in range(HALF_DEV):
                w_b = jnp.broadcast_to(w_s[leaf, r, pl.ds(t, 1), :], (16, 128)).astype(BF16)
                hi_b = jnp.broadcast_to(hi_s[leaf, r, pl.ds(t, 1), :], (16, 128)).astype(BF16)
                lo_b = jnp.broadcast_to(lo_s[leaf, r, pl.ds(t, 1), :], (16, 128)).astype(BF16)
                lhs.append(jnp.concatenate([jnp.where(hi_b == row16 + 16 * i, w_b, zero) for i in range(2)], axis=0))
                rhs.append(jnp.concatenate([jnp.where(lo_b == row16 + 16 * i, one, zero) for i in range(2)], axis=0))
            table = lax.dot_general(
                jnp.concatenate(lhs, axis=1),
                jnp.concatenate(rhs, axis=1),
                (((1,), (1,)), ((), ())),
                preferred_element_type=F32,
            )
            table_ref[leaf, t] = table
            sum_s[leaf, pl.ds(t, 1), :] = jnp.sum(table, axis=0, keepdims=True)
            top_s[leaf, pl.ds(t, 1), :] = jnp.max(table, axis=0, keepdims=True)
        return carry

    lax.fori_loop(0, GROUP, tree, 0, unroll=8)
    seen = jnp.zeros((GROUP, 1), F32)
    wrong = jnp.zeros((GROUP, 1), F32)
    for leaf in range(2):
        total = jnp.sum(sum_s[leaf], axis=1, keepdims=True)
        seen = seen + total
        wrong = wrong + (total - jnp.max(top_s[leaf], axis=1, keepdims=True))
    lane = lax.broadcasted_iota(I32, (GROUP, 128), 1)
    row = lax.broadcasted_iota(I32, (GROUP, 128), 0)
    placed = jnp.where(lane == row, wrong, 0.0) + jnp.where(lane == row + GROUP, seen, 0.0)
    message_ref[...] = jnp.broadcast_to(jnp.sum(placed, axis=0, keepdims=True), (N_DEV, 128))


def tally(received):
    return pl.pallas_call(
        tally_kernel,
        out_shape=(
            jax.ShapeDtypeStruct((2, GROUP, 32, 32), F32),
            jax.ShapeDtypeStruct((N_DEV, 128), F32),
        ),
        scratch_shapes=[pltpu.VMEM((2, HALF_DEV, GROUP, 128), F32)] * 3 + [pltpu.VMEM((2, GROUP, 32), F32)] * 2,
        compiler_params=pltpu.CompilerParams(vmem_limit_bytes=16 * 1024 * 1024),
        cost_estimate=pl.CostEstimate(flops=4_000_000_000, bytes_accessed=2_500_000, transcendentals=0),
        name="tally",
    )(received)


def errors_kernel(group_ref, in_ref, tree_ref, forest_ref):
    got = in_ref[...]
    source = lax.broadcasted_iota(I32, (N_DEV, 128), 0)
    mine = jnp.sum(jnp.where(source % N_TREES == group_ref[0], got, 0.0), axis=0, keepdims=True)
    every = jnp.sum(got, axis=0, keepdims=True)
    lane = lax.broadcasted_iota(I32, (1, 128), 1)
    wrong = jnp.sum(jnp.where(lane < GROUP, every, 0.0), axis=1, keepdims=True)
    seen = jnp.sum(jnp.where((lane >= GROUP) & (lane < 2 * GROUP), every, 0.0), axis=1, keepdims=True)
    ratio = mine / pltpu.roll(mine, 128 - GROUP, 1)
    tree_ref[...] = ratio[:, :GROUP]
    forest_ref[...] = wrong / seen


def errors(group, received):
    return pl.pallas_call(
        errors_kernel,
        in_specs=[pl.BlockSpec(memory_space=pltpu.SMEM), pl.BlockSpec(memory_space=pltpu.VMEM)],
        out_shape=(
            jax.ShapeDtypeStruct((1, GROUP), F32),
            jax.ShapeDtypeStruct((1, 1), F32),
        ),
        compiler_params=pltpu.CompilerParams(vmem_limit_bytes=4 * 1024 * 1024),
        name="errors",
    )(group, received)


def per_device(leaf_index, out_of_bag, labels):
    packed = pack(leaf_index, out_of_bag, labels).reshape(N_DEV, 2, GROUP, 128)
    received = lax.all_to_all(packed, ALL, 0, 0, tiled=True)
    table, message = tally(received)
    sums = lax.all_to_all(message, ALL, 0, 0, tiled=True)
    group = lax.axis_index(TREES).astype(I32).reshape(1)
    tree_error, forest_error = errors(group, sums)
    tallies = jnp.swapaxes(table.reshape(2, GROUP, 1024), 0, 1)[:, :, :CLASSES]
    return tallies, tree_error.reshape(GROUP), forest_error.reshape(())


def solution(mesh):
    split = Mesh(mesh.devices.reshape(4, 4, 4, 2), ALL)
    return jax.shard_map(
        per_device,
        mesh=split,
        in_specs=(P(None, ALL), P(None, ALL), P(ALL)),
        out_specs=(P(TREES, ROWS, None), P(TREES), P()),
        check_vma=False,
    )
```

```python
import jax
import jax.numpy as jnp
from jax import lax
from jax.experimental import pallas as pl
from jax.experimental.pallas import tpu as pltpu
from jax.sharding import Mesh
from jax.sharding import PartitionSpec as P

CLASSES = 1000
LEAVES = 32
TREES_ALL = 128
ROW_DEV = 2048
N_DEV = 128
N_ROWS = 16
N_TREES = 8
GROUP = TREES_ALL // N_TREES
RANKS = ROW_DEV // LEAVES
ROWS = ("rows_0", "rows_1")
TREES = ("trees_0", "trees_1")
ALL = ROWS + TREES
REGS = ROW_DEV // 8
HALF_DEV = N_DEV // 2

F32 = jnp.float32
BF16 = jnp.bfloat16
I32 = jnp.int32


def ordered(x, i, j):
    x[i], x[j] = jnp.minimum(x[i], x[j]), jnp.maximum(x[i], x[j])


LEAF_STEP = float(1 << 20)


def sort_key(leaf_index, out_of_bag):
    w = out_of_bag.astype(F32) * 512.0
    code = jnp.minimum(jnp.minimum(w, w * 0.5 + 128.0), jnp.minimum(w * 0.25 + 256.0, w * 0.125 + 384.0))
    code = lax.optimization_barrier(code)
    return (leaf_index - 16).astype(F32) * LEAF_STEP + code * 1024.0


def pack_kernel(key_ref, lab_ref, out_ref, s_ref):
    sub = lax.broadcasted_iota(I32, (8, 128), 0)

    def get(v):
        return s_ref[pl.ds(pl.multiple_of(v * 8, 8), 8), :]

    def put(v, x):
        s_ref[pl.ds(pl.multiple_of(v * 8, 8), 8), :] = x

    def sort_32(b, carry):
        x = [get(b * 32 + r) for r in range(32)]
        for k in range(1, 6):
            for i in range(32):
                j = i ^ ((1 << k) - 1)
                if i < j:
                    ordered(x, i, j)
            for d in reversed(range(k - 1)):
                for i in range(32):
                    if not i & (1 << d):
                        ordered(x, i, i | (1 << d))
        for r in range(32):
            put(b * 32 + r, x[r])
        return carry

    for c in range(ROW_DEV // 128):
        cols = pl.ds(c * 128, 128)
        s_ref[cols, :] = jnp.transpose(key_ref[:, cols] + lab_ref[:, cols].astype(F32))
    lax.fori_loop(0, REGS // 32, sort_32, 0, unroll=True)

    def low_bits(b, carry):
        x = [get(b * 32 + r) for r in range(32)]
        for d in reversed(range(5)):
            for i in range(32):
                if not i & (1 << d):
                    ordered(x, i, i | (1 << d))
        for r in range(32):
            put(b * 32 + r, x[r])
        return carry

    def swapped(x, flip):
        return jnp.take_along_axis(x, sub ^ flip, axis=0, mode="promise_in_bounds")

    def across(x, y, bit):
        return jnp.where(sub & bit == 0, jnp.minimum(x, y), jnp.maximum(x, y))

    def high_bits(k):
        top = min(k, 8)
        bits = list(range(5, top))
        n = 1 << len(bits)
        per_block = 16
        blocks = REGS >> top

        def body(t, carry):
            block, low = t // per_block, t % per_block
            base = block << top
            at = [base + (h << 5) + low for h in range(n)] + [base + (h << 5) + (31 - low) for h in range(n)]
            x = [get(v) for v in at]
            mirror = lambda e: (n - 1 - e % n) + (n if e < n else 0)
            if k <= 8:
                for e in range(n):
                    if e & (n >> 1):
                        continue
                    ordered(x, e, mirror(e))
                    ordered(x, e + n, mirror(e + n))
            else:
                flip = (1 << (k - 8)) - 1
                x = [across(x[e], swapped(x[mirror(e)], flip), 1 << (k - 9)) for e in range(2 * n)]
                for d in reversed(range(k - 9)):
                    x = [across(v, swapped(v, 1 << d), 1 << d) for v in x]
            first = len(bits) - 2 if k <= 8 else len(bits) - 1
            for d in reversed(range(1 if k == 11 else 0, first + 1)):
                for e in range(2 * n):
                    if not e & (1 << d):
                        ordered(x, e, e | (1 << d))
            for v, val in zip(at, x):
                put(v, val)
            return carry

        lax.fori_loop(0, blocks * per_block, body, 0, unroll=True)

    for k in range(6, 11):
        high_bits(k)
        lax.fori_loop(0, REGS // 32, low_bits, 0, unroll=True)
    high_bits(11)

    odd = (lax.broadcasted_iota(I32, (1, 128), 1) >= RANKS).astype(F32)
    for p in range(N_ROWS):
        start = (p % 2) * 1024 + p // 2
        key = jnp.transpose(s_ref[pl.ds(start, 128, stride=8), :])
        rest = key - (odd + float(2 * p - 16)) * LEAF_STEP
        code = jnp.floor(rest * (1.0 / 1024.0))
        label = rest - code * 1024.0
        w = jnp.maximum(
            jnp.maximum(code, code * 2.0 - 256.0), jnp.maximum(code * 4.0 - 1024.0, code * 8.0 - 3072.0)
        ) * (1.0 / 512.0)
        out_ref[p, :, 0] = w.reshape(N_TREES, GROUP, 128)
        out_ref[p, :, 1] = label.reshape(N_TREES, GROUP, 128)


def pack(key, labels):
    return pl.pallas_call(
        pack_kernel,
        out_shape=jax.ShapeDtypeStruct((N_ROWS, N_TREES, 2, GROUP, 128), F32),
        scratch_shapes=[pltpu.VMEM((ROW_DEV, 128), F32)],
        compiler_params=pltpu.CompilerParams(vmem_limit_bytes=16 * 1024 * 1024),
        cost_estimate=pl.CostEstimate(flops=40_000_000, bytes_accessed=3_100_000, transcendentals=0),
        name="pack",
    )(key, labels.reshape(1, ROW_DEV))


def iota16(shape):
    return lax.broadcasted_iota(I32, shape, 0).astype(F32).astype(BF16)


TAG = 2 * GROUP


def tally_kernel(in_ref, tallies_ref, message_ref, w_s, hi_s, lo_s, flat_s, sum_s, top_s):
    low8 = lax.broadcasted_iota(I32, (8, 128), 1) < RANKS
    row16 = iota16((16, 128))
    quarter = lax.broadcasted_iota(I32, (32, 128), 0) % 4
    zero = jnp.zeros((16, 128), BF16)
    one = jnp.ones((16, 128), BF16)

    def halves(a, b):
        return (
            jnp.where(low8, a, pltpu.roll(b, RANKS, 1)),
            jnp.where(low8, pltpu.roll(a, RANKS, 1), b),
        )

    def spread(octet, s):
        trees = pl.ds(8 * octet, 8)
        w2 = halves(in_ref[s, 0, trees, :], in_ref[s + HALF_DEV, 0, trees, :])
        lab2 = halves(in_ref[s, 1, trees, :], in_ref[s + HALF_DEV, 1, trees, :])
        for leaf in range(2):
            hi = jnp.floor(lab2[leaf] * (1.0 / 32.0))
            w_s[octet, leaf, s] = w2[leaf]
            hi_s[octet, leaf, s] = hi
            lo_s[octet, leaf, s] = lab2[leaf] - 32.0 * hi

    def tree(t):
        octet, u = divmod(t, 8)
        for leaf in range(2):
            lhs, rhs = [], []
            for r in range(HALF_DEV):
                w_b = jnp.broadcast_to(w_s[octet, leaf, r, u : u + 1, :], (16, 128)).astype(BF16)
                hi_b = jnp.broadcast_to(hi_s[octet, leaf, r, u : u + 1, :], (16, 128)).astype(BF16)
                lo_b = jnp.broadcast_to(lo_s[octet, leaf, r, u : u + 1, :], (16, 128)).astype(BF16)
                lhs.append(jnp.concatenate([jnp.where(hi_b == row16 + 16 * i, w_b, zero) for i in range(2)], axis=0))
                rhs.append(jnp.concatenate([jnp.where(lo_b == row16 + 16 * i, one, zero) for i in range(2)], axis=0))
            table = lax.dot_general(
                jnp.concatenate(lhs, axis=1),
                jnp.concatenate(rhs, axis=1),
                (((1,), (1,)), ((), ())),
                preferred_element_type=F32,
            )
            sum_s[leaf, t : t + 1, :] = jnp.sum(table, axis=0, keepdims=True)
            top_s[leaf, t : t + 1, :] = jnp.max(table, axis=0, keepdims=True)
            wide = jnp.concatenate([table, jnp.zeros((32, 96), F32)], axis=1)
            placed = wide
            for j in range(1, 4):
                placed = jnp.where(quarter == j, pltpu.roll(wide, 32 * j, 1), placed)
            flat_s[t, leaf] = placed
            rows = flat_s[t, leaf, pl.ds(0, 8, stride=4), :]
            for j in range(1, 4):
                rows = rows + flat_s[t, leaf, pl.ds(j, 8, stride=4), :]
            for k in range(8):
                width = min(128, CLASSES - 128 * k)
                tallies_ref[t, leaf : leaf + 1, 128 * k : 128 * k + width] = rows[k : k + 1, :width]

    for s in range(HALF_DEV):
        spread(0, s)
    for t in range(8):
        for s in range(8 * t, 8 * t + 8):
            spread(1, s)
        tree(t)
    for t in range(8, GROUP):
        tree(t)
    seen = jnp.zeros((GROUP, 1), F32)
    wrong = jnp.zeros((GROUP, 1), F32)
    for leaf in range(2):
        total = jnp.sum(sum_s[leaf], axis=1, keepdims=True)
        seen = seen + total
        wrong = wrong + (total - jnp.max(top_s[leaf], axis=1, keepdims=True))
    lane = lax.broadcasted_iota(I32, (GROUP, 128), 1)
    row = lax.broadcasted_iota(I32, (GROUP, 128), 0)
    placed = jnp.where(lane == row, wrong, 0.0) + jnp.where(lane == row + GROUP, seen, 0.0)
    sums = jnp.broadcast_to(jnp.sum(placed, axis=0, keepdims=True), (N_DEV, 128))
    receiver = (lax.broadcasted_iota(I32, (N_DEV, 128), 0) % N_TREES).astype(F32)
    message_ref[...] = jnp.where(lax.broadcasted_iota(I32, (N_DEV, 128), 1) == TAG, receiver, sums)


def tally(received):
    return pl.pallas_call(
        tally_kernel,
        out_shape=(
            jax.ShapeDtypeStruct((GROUP, 2, CLASSES), F32),
            jax.ShapeDtypeStruct((N_DEV, 128), F32),
        ),
        scratch_shapes=[pltpu.VMEM((2, 2, HALF_DEV, 8, 128), F32)] * 3
        + [pltpu.VMEM((GROUP, 2, 32, 128), F32)]
        + [pltpu.VMEM((2, GROUP, 32), F32)] * 2,
        compiler_params=pltpu.CompilerParams(vmem_limit_bytes=16 * 1024 * 1024),
        cost_estimate=pl.CostEstimate(flops=4_000_000_000, bytes_accessed=2_500_000, transcendentals=0),
        name="tally",
    )(received)


def errors_kernel(in_ref, tree_ref, forest_ref):
    got = in_ref[...]
    source = (lax.broadcasted_iota(I32, (N_DEV, 128), 0) % N_TREES).astype(F32)
    mine = jnp.sum(jnp.where(source == got[:, TAG : TAG + 1], got, 0.0), axis=0, keepdims=True)
    every = jnp.sum(got, axis=0, keepdims=True)
    lane = lax.broadcasted_iota(I32, (1, 128), 1)
    wrong = jnp.sum(jnp.where(lane < GROUP, every, 0.0), axis=1, keepdims=True)
    seen = jnp.sum(jnp.where((lane >= GROUP) & (lane < 2 * GROUP), every, 0.0), axis=1, keepdims=True)
    ratio = mine / pltpu.roll(mine, 128 - GROUP, 1)
    tree_ref[...] = ratio[:, :GROUP]
    forest_ref[...] = wrong / seen


def errors(received):
    return pl.pallas_call(
        errors_kernel,
        out_shape=(
            jax.ShapeDtypeStruct((1, GROUP), F32),
            jax.ShapeDtypeStruct((1, 1), F32),
        ),
        compiler_params=pltpu.CompilerParams(vmem_limit_bytes=4 * 1024 * 1024),
        name="errors",
    )(received)


def per_device(leaf_index, out_of_bag, labels):
    packed = pack(sort_key(leaf_index, out_of_bag), labels).reshape(N_DEV, 2, GROUP, 128)
    received = lax.all_to_all(packed, ALL, 0, 0, tiled=True)
    tallies, message = tally(received)
    sums = lax.all_to_all(message, ALL, 0, 0, tiled=True)
    tree_error, forest_error = errors(sums)
    return tallies, tree_error.reshape(GROUP), forest_error.reshape(())


def solution(mesh):
    split = Mesh(mesh.devices.reshape(4, 4, 4, 2), ALL)
    return jax.shard_map(
        per_device,
        mesh=split,
        in_specs=(P(None, ALL), P(None, ALL), P(ALL)),
        out_specs=(P(TREES, ROWS, None), P(TREES), P()),
        check_vma=False,
    )
```

```python
import jax
import jax.numpy as jnp
from jax import lax
from jax.experimental import pallas as pl
from jax.experimental.pallas import tpu as pltpu
from jax.sharding import Mesh
from jax.sharding import PartitionSpec as P

CLASSES = 1000
LEAVES = 32
TREES_ALL = 128
ROW_DEV = 2048
N_DEV = 128
N_ROWS = 16
N_TREES = 8
GROUP = TREES_ALL // N_TREES
RANKS = ROW_DEV // LEAVES
ROWS = ("rows_0", "rows_1")
TREES = ("trees_0", "trees_1")
ALL = ROWS + TREES
REGS = ROW_DEV // 8
HALF_DEV = N_DEV // 2

F32 = jnp.float32
BF16 = jnp.bfloat16
I32 = jnp.int32


def ordered(x, i, j):
    x[i], x[j] = jnp.minimum(x[i], x[j]), jnp.maximum(x[i], x[j])


LEAF_STEP = float(1 << 20)


def sort_key(leaf_index, out_of_bag):
    w = out_of_bag.astype(F32) * 512.0
    code = jnp.minimum(jnp.minimum(w, w * 0.5 + 128.0), jnp.minimum(w * 0.25 + 256.0, w * 0.125 + 384.0))
    code = lax.optimization_barrier(code)
    return (leaf_index - 16).astype(F32) * LEAF_STEP + code * 1024.0


def pack_kernel(key_ref, lab_ref, out_ref, s_ref):
    sub = lax.broadcasted_iota(I32, (8, 128), 0)

    def get(v):
        return s_ref[pl.ds(pl.multiple_of(v * 8, 8), 8), :]

    def put(v, x):
        s_ref[pl.ds(pl.multiple_of(v * 8, 8), 8), :] = x

    def sort_32(b, carry):
        x = [get(b * 32 + r) for r in range(32)]
        for k in range(1, 6):
            for i in range(32):
                j = i ^ ((1 << k) - 1)
                if i < j:
                    ordered(x, i, j)
            for d in reversed(range(k - 1)):
                for i in range(32):
                    if not i & (1 << d):
                        ordered(x, i, i | (1 << d))
        for r in range(32):
            put(b * 32 + r, x[r])
        return carry

    for c in range(ROW_DEV // 128):
        cols = pl.ds(c * 128, 128)
        s_ref[cols, :] = jnp.transpose(key_ref[:, cols] + lab_ref[:, cols].astype(F32))
    lax.fori_loop(0, REGS // 32, sort_32, 0, unroll=True)

    def low_bits(b, carry):
        x = [get(b * 32 + r) for r in range(32)]
        for d in reversed(range(5)):
            for i in range(32):
                if not i & (1 << d):
                    ordered(x, i, i | (1 << d))
        for r in range(32):
            put(b * 32 + r, x[r])
        return carry

    def swapped(x, flip):
        return jnp.take_along_axis(x, sub ^ flip, axis=0, mode="promise_in_bounds")

    def across(x, y, bit):
        return jnp.where(sub & bit == 0, jnp.minimum(x, y), jnp.maximum(x, y))

    def high_bits(k):
        top = min(k, 8)
        bits = list(range(5, top))
        n = 1 << len(bits)
        per_block = 16
        blocks = REGS >> top

        def body(t, carry):
            block, low = t // per_block, t % per_block
            base = block << top
            at = [base + (h << 5) + low for h in range(n)] + [base + (h << 5) + (31 - low) for h in range(n)]
            x = [get(v) for v in at]
            mirror = lambda e: (n - 1 - e % n) + (n if e < n else 0)
            if k <= 8:
                for e in range(n):
                    if e & (n >> 1):
                        continue
                    ordered(x, e, mirror(e))
                    ordered(x, e + n, mirror(e + n))
            else:
                flip = (1 << (k - 8)) - 1
                x = [across(x[e], swapped(x[mirror(e)], flip), 1 << (k - 9)) for e in range(2 * n)]
                for d in reversed(range(k - 9)):
                    x = [across(v, swapped(v, 1 << d), 1 << d) for v in x]
            first = len(bits) - 2 if k <= 8 else len(bits) - 1
            for d in reversed(range(1 if k == 11 else 0, first + 1)):
                for e in range(2 * n):
                    if not e & (1 << d):
                        ordered(x, e, e | (1 << d))
            for v, val in zip(at, x):
                put(v, val)
            return carry

        lax.fori_loop(0, blocks * per_block, body, 0, unroll=True)

    for k in range(6, 11):
        high_bits(k)
        lax.fori_loop(0, REGS // 32, low_bits, 0, unroll=True)
    high_bits(11)

    odd = (lax.broadcasted_iota(I32, (1, 128), 1) >= RANKS).astype(F32)
    for p in range(N_ROWS):
        start = (p % 2) * 1024 + p // 2
        key = jnp.transpose(s_ref[pl.ds(start, 128, stride=8), :])
        rest = key - (odd + float(2 * p - 16)) * LEAF_STEP
        code = jnp.floor(rest * (1.0 / 1024.0))
        label = rest - code * 1024.0
        w = jnp.maximum(
            jnp.maximum(code, code * 2.0 - 256.0), jnp.maximum(code * 4.0 - 1024.0, code * 8.0 - 3072.0)
        ) * (1.0 / 512.0)
        out_ref[p, :, 0] = w.reshape(N_TREES, GROUP, 128)
        out_ref[p, :, 1] = label.reshape(N_TREES, GROUP, 128)


def pack(key, labels):
    return pl.pallas_call(
        pack_kernel,
        out_shape=jax.ShapeDtypeStruct((N_ROWS, N_TREES, 2, GROUP, 128), F32),
        scratch_shapes=[pltpu.VMEM((ROW_DEV, 128), F32)],
        compiler_params=pltpu.CompilerParams(vmem_limit_bytes=16 * 1024 * 1024),
        cost_estimate=pl.CostEstimate(flops=40_000_000, bytes_accessed=3_100_000, transcendentals=0),
        name="pack",
    )(key, labels.reshape(1, ROW_DEV))


def iota16(shape):
    return lax.broadcasted_iota(I32, shape, 0).astype(F32).astype(BF16)


TAG = 2 * GROUP


def tally_kernel(in_ref, tallies_ref, message_ref, w_s, hi_s, lo_s, flat_s, sum_s, top_s):
    low8 = lax.broadcasted_iota(I32, (8, 128), 1) < RANKS
    row16 = iota16((16, 128))
    quarter = lax.broadcasted_iota(I32, (32, 128), 0) % 4
    zero = jnp.zeros((16, 128), BF16)
    one = jnp.ones((16, 128), BF16)

    def halves(a, b):
        return (
            jnp.where(low8, a, pltpu.roll(b, RANKS, 1)),
            jnp.where(low8, pltpu.roll(a, RANKS, 1), b),
        )

    def spread(octet, s):
        trees = pl.ds(8 * octet, 8)
        w2 = halves(in_ref[s, 0, trees, :], in_ref[s + HALF_DEV, 0, trees, :])
        lab2 = halves(in_ref[s, 1, trees, :], in_ref[s + HALF_DEV, 1, trees, :])
        for leaf in range(2):
            hi = jnp.floor(lab2[leaf] * (1.0 / 32.0))
            w_s[octet, leaf, s] = w2[leaf]
            hi_s[octet, leaf, s] = hi
            lo_s[octet, leaf, s] = lab2[leaf] - 32.0 * hi

    def tree(t):
        octet, u = divmod(t, 8)
        for leaf in range(2):
            lhs, rhs = [], []
            for r in range(HALF_DEV):
                w_b = jnp.broadcast_to(w_s[octet, leaf, r, u : u + 1, :], (16, 128)).astype(BF16)
                hi_b = jnp.broadcast_to(hi_s[octet, leaf, r, u : u + 1, :], (16, 128)).astype(BF16)
                lo_b = jnp.broadcast_to(lo_s[octet, leaf, r, u : u + 1, :], (16, 128)).astype(BF16)
                lhs.append(jnp.concatenate([jnp.where(hi_b == row16 + 16 * i, w_b, zero) for i in range(2)], axis=0))
                rhs.append(jnp.concatenate([jnp.where(lo_b == row16 + 16 * i, one, zero) for i in range(2)], axis=0))
            table = lax.dot_general(
                jnp.concatenate(lhs, axis=1),
                jnp.concatenate(rhs, axis=1),
                (((1,), (1,)), ((), ())),
                preferred_element_type=F32,
            )
            sum_s[leaf, t : t + 1, :] = jnp.sum(table, axis=0, keepdims=True)
            top_s[leaf, t : t + 1, :] = jnp.max(table, axis=0, keepdims=True)
            wide = jnp.concatenate([table, jnp.zeros((32, 96), F32)], axis=1)
            placed = wide
            for j in range(1, 4):
                placed = jnp.where(quarter == j, pltpu.roll(wide, 32 * j, 1), placed)
            flat_s[t, leaf] = placed
            rows = flat_s[t, leaf, pl.ds(0, 8, stride=4), :]
            for j in range(1, 4):
                rows = rows + flat_s[t, leaf, pl.ds(j, 8, stride=4), :]
            for k in range(8):
                width = min(128, CLASSES - 128 * k)
                tallies_ref[t, leaf : leaf + 1, 128 * k : 128 * k + width] = rows[k : k + 1, :width]

    for s in range(HALF_DEV):
        spread(0, s)
    for t in range(8):
        for s in range(8 * t, 8 * t + 8):
            spread(1, s)
        tree(t)
    for t in range(8, GROUP):
        tree(t)
    seen = jnp.zeros((GROUP, 1), F32)
    wrong = jnp.zeros((GROUP, 1), F32)
    for leaf in range(2):
        total = jnp.sum(sum_s[leaf], axis=1, keepdims=True)
        seen = seen + total
        wrong = wrong + (total - jnp.max(top_s[leaf], axis=1, keepdims=True))
    lane = lax.broadcasted_iota(I32, (GROUP, 128), 1)
    row = lax.broadcasted_iota(I32, (GROUP, 128), 0)
    placed = jnp.where(lane == row, wrong, 0.0) + jnp.where(lane == row + GROUP, seen, 0.0)
    sums = jnp.broadcast_to(jnp.sum(placed, axis=0, keepdims=True), (N_DEV, 128))
    receiver = (lax.broadcasted_iota(I32, (N_DEV, 128), 0) % N_TREES).astype(F32)
    message_ref[...] = jnp.where(lax.broadcasted_iota(I32, (N_DEV, 128), 1) == TAG, receiver, sums)


def tally(received):
    return pl.pallas_call(
        tally_kernel,
        out_shape=(
            jax.ShapeDtypeStruct((GROUP, 2, CLASSES), F32),
            jax.ShapeDtypeStruct((N_DEV, 128), F32),
        ),
        scratch_shapes=[pltpu.VMEM((2, 2, HALF_DEV, 8, 128), F32)] * 3
        + [pltpu.VMEM((GROUP, 2, 32, 128), F32)]
        + [pltpu.VMEM((2, GROUP, 32), F32)] * 2,
        compiler_params=pltpu.CompilerParams(vmem_limit_bytes=16 * 1024 * 1024),
        cost_estimate=pl.CostEstimate(flops=4_000_000_000, bytes_accessed=2_500_000, transcendentals=0),
        name="tally",
    )(received)


def errors_kernel(in_ref, made_ref, tallies_ref, tree_ref, forest_ref):
    tallies_ref[...] = made_ref[...]
    got = in_ref[...]
    source = (lax.broadcasted_iota(I32, (N_DEV, 128), 0) % N_TREES).astype(F32)
    mine = jnp.sum(jnp.where(source == got[:, TAG : TAG + 1], got, 0.0), axis=0, keepdims=True)
    every = jnp.sum(got, axis=0, keepdims=True)
    lane = lax.broadcasted_iota(I32, (1, 128), 1)
    wrong = jnp.sum(jnp.where(lane < GROUP, every, 0.0), axis=1, keepdims=True)
    seen = jnp.sum(jnp.where((lane >= GROUP) & (lane < 2 * GROUP), every, 0.0), axis=1, keepdims=True)
    ratio = mine / pltpu.roll(mine, 128 - GROUP, 1)
    tree_ref[...] = ratio[:, :GROUP]
    forest_ref[...] = wrong / seen


def errors(received, tallies):
    return pl.pallas_call(
        errors_kernel,
        out_shape=(
            jax.ShapeDtypeStruct((GROUP, 2, CLASSES), F32),
            jax.ShapeDtypeStruct((1, GROUP), F32),
            jax.ShapeDtypeStruct((1, 1), F32),
        ),
        compiler_params=pltpu.CompilerParams(vmem_limit_bytes=4 * 1024 * 1024),
        name="errors",
    )(received, tallies)


def per_device(leaf_index, out_of_bag, labels):
    packed = pack(sort_key(leaf_index, out_of_bag), labels).reshape(N_DEV, 2, GROUP, 128)
    received = lax.all_to_all(packed, ALL, 0, 0, tiled=True)
    tallies, message = tally(received)
    sums = lax.all_to_all(message, ALL, 0, 0, tiled=True)
    tallies, tree_error, forest_error = errors(sums, tallies)
    return tallies, tree_error.reshape(GROUP), forest_error.reshape(())


def solution(mesh):
    split = Mesh(mesh.devices.reshape(4, 4, 4, 2), ALL)
    return jax.shard_map(
        per_device,
        mesh=split,
        in_specs=(P(None, ALL), P(None, ALL), P(ALL)),
        out_specs=(P(TREES, ROWS, None), P(TREES), P()),
        check_vma=False,
    )
```

```python
import jax
import jax.numpy as jnp
from jax import lax
from jax.experimental import pallas as pl
from jax.experimental.pallas import tpu as pltpu
from jax.sharding import Mesh
from jax.sharding import PartitionSpec as P

CLASSES = 1000
LEAVES = 32
TREES_ALL = 128
ROW_DEV = 2048
N_DEV = 128
N_ROWS = 16
N_TREES = 8
GROUP = TREES_ALL // N_TREES
RANKS = ROW_DEV // LEAVES
ROWS = ("rows_0", "rows_1")
TREES = ("trees_0", "trees_1")
ALL = ROWS + TREES
REGS = ROW_DEV // 8
HALF_DEV = N_DEV // 2

F32 = jnp.float32
BF16 = jnp.bfloat16
I32 = jnp.int32


def odd_even(n):
    p = 1
    while p < n:
        k = p
        while k:
            for j in range(k % p, n - k, 2 * k):
                for i in range(min(k, n - j - k)):
                    if (i + j) // (2 * p) == (i + j + k) // (2 * p):
                        yield i + j, i + j + k
            k //= 2
        p *= 2


def ordered(x, i, j):
    x[i], x[j] = jnp.minimum(x[i], x[j]), jnp.maximum(x[i], x[j])


LEAF_STEP = float(1 << 20)


def sort_key(leaf_index, out_of_bag):
    w = out_of_bag.astype(F32) * 512.0
    code = jnp.minimum(jnp.minimum(w, w * 0.5 + 128.0), jnp.minimum(w * 0.25 + 256.0, w * 0.125 + 384.0))
    code = lax.optimization_barrier(code)
    return (leaf_index - 16).astype(F32) * LEAF_STEP + code * 1024.0


def pack_kernel(key_ref, lab_ref, out_ref, s_ref):
    sub = lax.broadcasted_iota(I32, (8, 128), 0)

    def get(v):
        return s_ref[pl.ds(pl.multiple_of(v * 8, 8), 8), :]

    def put(v, x):
        s_ref[pl.ds(pl.multiple_of(v * 8, 8), 8), :] = x

    def sort_32(b, carry):
        x = [get(b * 32 + r) for r in range(32)]
        for i, j in odd_even(32):
            ordered(x, i, j)
        for r in range(32):
            put(b * 32 + r, x[r])
        return carry

    for c in range(ROW_DEV // 128):
        cols = pl.ds(c * 128, 128)
        s_ref[cols, :] = jnp.transpose(key_ref[:, cols] + lab_ref[:, cols].astype(F32))
    lax.fori_loop(0, REGS // 32, sort_32, 0, unroll=True)

    def low_bits(b, carry):
        x = [get(b * 32 + r) for r in range(32)]
        for d in reversed(range(5)):
            for i in range(32):
                if not i & (1 << d):
                    ordered(x, i, i | (1 << d))
        for r in range(32):
            put(b * 32 + r, x[r])
        return carry

    def swapped(x, flip):
        return jnp.take_along_axis(x, sub ^ flip, axis=0, mode="promise_in_bounds")

    def across(x, y, bit):
        return jnp.where(sub & bit == 0, jnp.minimum(x, y), jnp.maximum(x, y))

    def high_bits(k):
        top = min(k, 8)
        bits = list(range(5, top))
        n = 1 << len(bits)
        per_block = 16
        blocks = REGS >> top

        def body(t, carry):
            block, low = t // per_block, t % per_block
            base = block << top
            at = [base + (h << 5) + low for h in range(n)] + [base + (h << 5) + (31 - low) for h in range(n)]
            x = [get(v) for v in at]
            mirror = lambda e: (n - 1 - e % n) + (n if e < n else 0)
            if k <= 8:
                for e in range(n):
                    if e & (n >> 1):
                        continue
                    ordered(x, e, mirror(e))
                    ordered(x, e + n, mirror(e + n))
            else:
                flip = (1 << (k - 8)) - 1
                x = [across(x[e], swapped(x[mirror(e)], flip), 1 << (k - 9)) for e in range(2 * n)]
                for d in reversed(range(k - 9)):
                    x = [across(v, swapped(v, 1 << d), 1 << d) for v in x]
            first = len(bits) - 2 if k <= 8 else len(bits) - 1
            for d in reversed(range(1 if k == 11 else 0, first + 1)):
                for e in range(2 * n):
                    if not e & (1 << d):
                        ordered(x, e, e | (1 << d))
            for v, val in zip(at, x):
                put(v, val)
            return carry

        lax.fori_loop(0, blocks * per_block, body, 0, unroll=True)

    for k in range(6, 11):
        high_bits(k)
        lax.fori_loop(0, REGS // 32, low_bits, 0, unroll=True)
    high_bits(11)

    odd = (lax.broadcasted_iota(I32, (1, 128), 1) >= RANKS).astype(F32)
    for p in range(N_ROWS):
        start = (p % 2) * 1024 + p // 2
        key = jnp.transpose(s_ref[pl.ds(start, 128, stride=8), :])
        rest = key - (odd + float(2 * p - 16)) * LEAF_STEP
        code = jnp.floor(rest * (1.0 / 1024.0))
        label = rest - code * 1024.0
        w = jnp.maximum(
            jnp.maximum(code, code * 2.0 - 256.0), jnp.maximum(code * 4.0 - 1024.0, code * 8.0 - 3072.0)
        ) * (1.0 / 512.0)
        out_ref[p, :, 0] = w.reshape(N_TREES, GROUP, 128)
        out_ref[p, :, 1] = label.reshape(N_TREES, GROUP, 128)


def pack(key, labels):
    return pl.pallas_call(
        pack_kernel,
        out_shape=jax.ShapeDtypeStruct((N_ROWS, N_TREES, 2, GROUP, 128), F32),
        scratch_shapes=[pltpu.VMEM((ROW_DEV, 128), F32)],
        compiler_params=pltpu.CompilerParams(vmem_limit_bytes=16 * 1024 * 1024),
        cost_estimate=pl.CostEstimate(flops=40_000_000, bytes_accessed=3_100_000, transcendentals=0),
        name="pack",
    )(key, labels.reshape(1, ROW_DEV))


def iota16(shape):
    return lax.broadcasted_iota(I32, shape, 0).astype(F32).astype(BF16)


TAG = 2 * GROUP


def tally_kernel(in_ref, tallies_ref, message_ref, w_s, hi_s, lo_s, flat_s, sum_s, top_s):
    low8 = lax.broadcasted_iota(I32, (8, 128), 1) < RANKS
    row16 = iota16((16, 128))
    quarter = lax.broadcasted_iota(I32, (32, 128), 0) % 4
    zero = jnp.zeros((16, 128), BF16)
    one = jnp.ones((16, 128), BF16)

    def halves(a, b):
        return (
            jnp.where(low8, a, pltpu.roll(b, RANKS, 1)),
            jnp.where(low8, pltpu.roll(a, RANKS, 1), b),
        )

    def spread(octet, s):
        trees = pl.ds(8 * octet, 8)
        w2 = halves(in_ref[s, 0, trees, :], in_ref[s + HALF_DEV, 0, trees, :])
        lab2 = halves(in_ref[s, 1, trees, :], in_ref[s + HALF_DEV, 1, trees, :])
        for leaf in range(2):
            hi = jnp.floor(lab2[leaf] * (1.0 / 32.0))
            w_s[octet, leaf, s] = w2[leaf]
            hi_s[octet, leaf, s] = hi
            lo_s[octet, leaf, s] = lab2[leaf] - 32.0 * hi

    def tree(t):
        octet, u = divmod(t, 8)
        for leaf in range(2):
            lhs, rhs = [], []
            for r in range(HALF_DEV):
                w_b = jnp.broadcast_to(w_s[octet, leaf, r, u : u + 1, :], (16, 128)).astype(BF16)
                hi_b = jnp.broadcast_to(hi_s[octet, leaf, r, u : u + 1, :], (16, 128)).astype(BF16)
                lo_b = jnp.broadcast_to(lo_s[octet, leaf, r, u : u + 1, :], (16, 128)).astype(BF16)
                lhs.append(jnp.concatenate([jnp.where(hi_b == row16 + 16 * i, w_b, zero) for i in range(2)], axis=0))
                rhs.append(jnp.concatenate([jnp.where(lo_b == row16 + 16 * i, one, zero) for i in range(2)], axis=0))
            table = lax.dot_general(
                jnp.concatenate(lhs, axis=1),
                jnp.concatenate(rhs, axis=1),
                (((1,), (1,)), ((), ())),
                preferred_element_type=F32,
            )
            sum_s[leaf, t : t + 1, :] = jnp.sum(table, axis=0, keepdims=True)
            top_s[leaf, t : t + 1, :] = jnp.max(table, axis=0, keepdims=True)
            wide = jnp.concatenate([table, jnp.zeros((32, 96), F32)], axis=1)
            placed = wide
            for j in range(1, 4):
                placed = jnp.where(quarter == j, pltpu.roll(wide, 32 * j, 1), placed)
            flat_s[t, leaf] = placed
            rows = flat_s[t, leaf, pl.ds(0, 8, stride=4), :]
            for j in range(1, 4):
                rows = rows + flat_s[t, leaf, pl.ds(j, 8, stride=4), :]
            for k in range(8):
                width = min(128, CLASSES - 128 * k)
                tallies_ref[t, leaf : leaf + 1, 128 * k : 128 * k + width] = rows[k : k + 1, :width]

    for s in range(HALF_DEV):
        spread(0, s)
    for t in range(8):
        for s in range(8 * t, 8 * t + 8):
            spread(1, s)
        tree(t)
    for t in range(8, GROUP):
        tree(t)
    seen = jnp.zeros((GROUP, 1), F32)
    wrong = jnp.zeros((GROUP, 1), F32)
    for leaf in range(2):
        total = jnp.sum(sum_s[leaf], axis=1, keepdims=True)
        seen = seen + total
        wrong = wrong + (total - jnp.max(top_s[leaf], axis=1, keepdims=True))
    lane = lax.broadcasted_iota(I32, (GROUP, 128), 1)
    row = lax.broadcasted_iota(I32, (GROUP, 128), 0)
    placed = jnp.where(lane == row, wrong, 0.0) + jnp.where(lane == row + GROUP, seen, 0.0)
    sums = jnp.broadcast_to(jnp.sum(placed, axis=0, keepdims=True), (N_DEV, 128))
    receiver = (lax.broadcasted_iota(I32, (N_DEV, 128), 0) % N_TREES).astype(F32)
    message_ref[...] = jnp.where(lax.broadcasted_iota(I32, (N_DEV, 128), 1) == TAG, receiver, sums)


def tally(received):
    return pl.pallas_call(
        tally_kernel,
        out_shape=(
            jax.ShapeDtypeStruct((GROUP, 2, CLASSES), F32),
            jax.ShapeDtypeStruct((N_DEV, 128), F32),
        ),
        scratch_shapes=[pltpu.VMEM((2, 2, HALF_DEV, 8, 128), F32)] * 3
        + [pltpu.VMEM((GROUP, 2, 32, 128), F32)]
        + [pltpu.VMEM((2, GROUP, 32), F32)] * 2,
        compiler_params=pltpu.CompilerParams(vmem_limit_bytes=16 * 1024 * 1024),
        cost_estimate=pl.CostEstimate(flops=4_000_000_000, bytes_accessed=2_500_000, transcendentals=0),
        name="tally",
    )(received)


def errors_kernel(in_ref, made_ref, tallies_ref, tree_ref, forest_ref):
    tallies_ref[...] = made_ref[...]
    got = in_ref[...]
    source = (lax.broadcasted_iota(I32, (N_DEV, 128), 0) % N_TREES).astype(F32)
    mine = jnp.sum(jnp.where(source == got[:, TAG : TAG + 1], got, 0.0), axis=0, keepdims=True)
    every = jnp.sum(got, axis=0, keepdims=True)
    lane = lax.broadcasted_iota(I32, (1, 128), 1)
    wrong = jnp.sum(jnp.where(lane < GROUP, every, 0.0), axis=1, keepdims=True)
    seen = jnp.sum(jnp.where((lane >= GROUP) & (lane < 2 * GROUP), every, 0.0), axis=1, keepdims=True)
    ratio = mine / pltpu.roll(mine, 128 - GROUP, 1)
    tree_ref[...] = ratio[:, :GROUP]
    forest_ref[...] = wrong / seen


def errors(received, tallies):
    return pl.pallas_call(
        errors_kernel,
        out_shape=(
            jax.ShapeDtypeStruct((GROUP, 2, CLASSES), F32),
            jax.ShapeDtypeStruct((1, GROUP), F32),
            jax.ShapeDtypeStruct((1, 1), F32),
        ),
        compiler_params=pltpu.CompilerParams(vmem_limit_bytes=4 * 1024 * 1024),
        name="errors",
    )(received, tallies)


def per_device(leaf_index, out_of_bag, labels):
    packed = pack(sort_key(leaf_index, out_of_bag), labels).reshape(N_DEV, 2, GROUP, 128)
    received = lax.all_to_all(packed, ALL, 0, 0, tiled=True)
    tallies, message = tally(received)
    sums = lax.all_to_all(message, ALL, 0, 0, tiled=True)
    tallies, tree_error, forest_error = errors(sums, tallies)
    return tallies, tree_error.reshape(GROUP), forest_error.reshape(())


def solution(mesh):
    split = Mesh(mesh.devices.reshape(4, 4, 4, 2), ALL)
    return jax.shard_map(
        per_device,
        mesh=split,
        in_specs=(P(None, ALL), P(None, ALL), P(ALL)),
        out_specs=(P(TREES, ROWS, None), P(TREES), P()),
        check_vma=False,
    )
```
